512 devices in a mesh: ep: 128 (over y, z, core), dp: 4 (over x).
Axes of the slice: x: 4, y: 8, z: 8, core: 2. Of those that a mesh axis runs over, the one named last changes fastest.
Arguments:
- tokens: bfloat16 [8192, 3584], P(('ep', 'dp')), may hold values from -6 to 6
- norm_gain: float32 [3584], replicated, may hold values from 0.25 to 1.75
- router: bfloat16 [3584, 128], replicated, may hold values from -0.09375 to 0.09375
- next_router: bfloat16 [3584, 128], P('dp'), may hold values from -0.09375 to 0.09375
- expert_ids: int32 [8192, 8], P(('ep', 'dp')), may hold values from 0 to 127, all different within a row; in each aligned block of 16 rows (0 to 15, 16 to 31, ...) at most 2 rows name the same one
- store: bfloat16 [128, 4, 112, 128, 128], P('ep', 'dp'), may hold values from -0.125 to 0.125
- send_list: int32 [128, 128], P('ep'), may hold values from -1 to 111, as said below
- cache_map: int32 [128, 112], P('ep'), may hold values from 0 to 127, as said below
Outputs:
- layer_out: bfloat16 [8192, 3584], P(('ep', 'dp'))
- next_scores: float32 [8192, 128], P(('ep', 'dp'))
The draws below stay inside these ranges and needn't reach their ends.
Inputs may be any that keep to these rules, and one draw needn't show every extreme that they name: `expert_ids`: each row names 8 different experts; among the rows of one device no expert is named by more than 2 rows, a bound that some block reaches. `send_list`: an entry is -1 where that arriving slot stays empty; every row names each of the 112 store indices exactly once. `cache_map`: each entry numbers an arriving slot of that device that is never empty; the entries of a row are distinct.
All inputs are finite; a program needn't handle non-finite values.
Results may differ from the reference program's by a relative error of at most 0.0095.
Values may be sent and summed in bfloat16 or wider, within the bound.
A program may use at most 64 MiB of HBM per device.

```python
import math
import jax
import jax.numpy as jnp
import numpy as np
from jax import lax

D = 3584
FF = 1024
TOP = 8
TR = 128
TC = 128
TOK_DEV = 16
EXPERTS = 128
CAP = 2
TILES_DEV = 112
PB = 1
TOKENS = 8192
N_EP = 128
N_DP = 4


def tile_layout(key):
    count = N_EP * PB
    key_pairs, key_order, key_local = jax.random.split(jax.random.fold_in(key, 7), 3)
    pairs = jax.random.permutation(key_pairs, count)[:TILES_DEV]
    offsets = pairs // PB
    lanes = pairs % PB
    order = jax.random.permutation(key_order, N_EP)
    position = jnp.argsort(order)
    owner = order[(position[:, None] + offsets[None, :]) % N_EP]
    local_keys = jax.random.split(key_local, N_EP)
    local = jax.vmap(lambda single: jax.random.permutation(single, TILES_DEV))(local_keys)
    devices = jnp.arange(N_EP, dtype=jnp.int32)[:, None] + jnp.zeros((1, TILES_DEV), jnp.int32)
    columns = devices * PB + lanes[None, :]
    chosen = local[owner, jnp.arange(TILES_DEV, dtype=jnp.int32)[None, :]]
    listing = jnp.full((N_EP, count), -1, jnp.int32)
    listing = listing.at[owner.reshape(-1), columns.reshape(-1)].set(chosen.reshape(-1).astype(jnp.int32))
    mapping = (owner * PB + lanes[None, :]).astype(jnp.int32)
    return (listing, mapping)


def draw_send_list(key, part):
    return tile_layout(key)[0]


def draw_cache_map(key, part):
    return tile_layout(key)[1]


def levels(rng, shape, cuts, least, largest):
    def one(dim, shards_of):
        draws = jax.random.uniform(jax.random.fold_in(jax.random.fold_in(rng, 6), dim), (shards_of,), jnp.float32, least / len(cuts), largest / len(cuts))
        return jnp.repeat(jnp.exp(draws), shape[dim] // shards_of).reshape((-1,) + (1,) * (len(shape) - dim - 1))

    level = one(*cuts[0])
    for cut in cuts[1:]:
        level = level * one(*cut)
    return level


def routed_block(own_key, own, number, rows, count, top, most, lean):
    sequence = jax.random.permutation(own_key, count)
    packed, common = portions_of(count, rows * top, most, lean, True), portions_of(count, rows * top, most, lean, False)
    places = jnp.arange(count)

    def named(sizes, rotation):
        used = int((sizes > 0).sum())
        fixed = max(1, used // 4)
        shifted = fixed + (places - fixed + rotation * (used - fixed)) % max(1, count - fixed)
        return jnp.zeros((count,), jnp.int32).at[sequence[jnp.where(places < fixed, places, shifted)]].set(jnp.asarray(sizes, jnp.int32))

    sizes = jnp.where(number % 4 == 0, named(packed, number // 4), named(common, number - number // 4 - 1))
    mixed = jax.random.permutation(jax.random.fold_in(own, 3), count)
    source_of, taker = mixed[0:count // 2 * 2:2], mixed[1:count // 2 * 2:2]
    slack = jnp.minimum(sizes[source_of] - 1, most - sizes[taker]) // 2
    slack = jnp.where((source_of == sequence[0]) | (taker == sequence[0]) | (sizes[taker] == 0), 0, jnp.maximum(slack, 0))
    shifted = jax.random.randint(jax.random.fold_in(own, 4), (count // 2,), 0, 1 << 20) % (slack + 1)
    sizes = sizes.at[source_of].add(-shifted).at[taker].add(shifted)
    labels = jnp.searchsorted(jnp.cumsum(sizes), jnp.arange(rows * top), side="right").astype(jnp.int32)
    table = labels.reshape(top, rows).T
    table = table[jax.random.permutation(jax.random.fold_in(own, 1), rows)]
    rotation = jax.random.randint(jax.random.fold_in(own, 2), (rows, 1), 0, top)
    return jnp.take_along_axis(table, (jnp.arange(top)[None, :] + rotation) % top, axis=1)


def portions_of(amount, total, most, lean, full):
    portions = [(1 << 20) // math.isqrt(grade ** lean) + 1 for grade in range(1, amount + 1)]
    largest = most if full else min(most, max(-(-total // amount), total * portions[0] // sum(portions)))
    least = 1 if total - largest >= amount - 1 else 0
    holding, rest = [largest] + [least] * (amount - 1), total - largest - least * (amount - 1)
    while rest > 0:
        candidates = [i for i in range(1, amount) if holding[i] < largest] or [i for i in range(1, amount) if holding[i] < most]
        mass, remaining = sum([portions[i] for i in candidates]), rest
        for i in candidates:
            addition = min(most - holding[i], max(1, remaining * portions[i] // mass), rest)
            holding[i] = holding[i] + addition
            rest = rest - addition
    return np.array(holding)


def bell_draw(key, shape, scale, most, pieces=(), kind=jnp.bfloat16):
    drawn = scale * jax.random.normal(key, shape, jnp.float32)
    if pieces:
        drawn = drawn * levels(key, shape, pieces, -0.22, 0.18)
    return jnp.clip(drawn, -most, most).astype(kind)


def setup_inputs(seed: int = 0) -> dict:
    splits = jax.random.split(jax.random.key(seed), 9)
    tokens = bell_draw(splits[0], (TOKENS, D), 1.0, 6.0, ((0, 512),))
    norm_gain = jnp.clip(1.0 + 0.15 * jax.random.normal(splits[1], (D,), jnp.float32), 0.25, 1.75)
    router = bell_draw(splits[2], (D, EXPERTS), D ** -0.5, 0.09375)
    next_router = bell_draw(splits[3], (D, EXPERTS), D ** -0.5, 0.09375, ((0, 4),))
    expert_ids_keys = jax.random.split(jax.random.fold_in(splits[4], 1), TOKENS // TOK_DEV)
    expert_ids_turns = jax.random.permutation(jax.random.fold_in(splits[4], 3), TOKENS // TOK_DEV)
    expert_ids = jax.vmap(lambda own, number: routed_block(jax.random.fold_in(splits[4], 2), own, number, TOK_DEV, EXPERTS, TOP, CAP, 2))(expert_ids_keys, expert_ids_turns).reshape((TOKENS, TOP))
    store = bell_draw(splits[5], (N_EP, N_DP, TILES_DEV, TR, TC), (2 * FF) ** -0.5, 0.125, ((0, 128), (1, 4)))
    send_list = draw_send_list(jax.random.fold_in(splits[8], 71), 0)
    cache_map = draw_cache_map(jax.random.fold_in(splits[8], 71), 0)
    return dict(tokens=tokens, norm_gain=norm_gain, router=router, next_router=next_router, expert_ids=expert_ids, store=store, send_list=send_list, cache_map=cache_map)


def reference(tokens, norm_gain, router, next_router, expert_ids, store, send_list, cache_map):
    values = tokens.astype(jnp.float32)
    scale = lax.rsqrt(lax.optimization_barrier(jnp.mean(values * values, axis=1, keepdims=True)) + 1e-06)
    normed = (values * scale * norm_gain).astype(jnp.bfloat16)
    scores = jax.nn.sigmoid(jnp.dot(normed, router, preferred_element_type=jnp.float32))
    picked = jnp.take_along_axis(scores, expert_ids, axis=1)
    weights = (2.5 * picked / lax.optimization_barrier(jnp.sum(picked, axis=1, keepdims=True))).astype(jnp.bfloat16)
    count = tokens.shape[0]
    limit = N_DP * N_EP * CAP
    row_tiles = D // (N_DP * TR)
    col_tiles = FF // TC

    def one_expert(total, expert):
        mapping = cache_map[expert]
        owners = mapping // PB
        lanes = mapping % PB
        local = send_list[owners, expert * PB + lanes]
        blocks = []
        for group in range(N_DP):
            tiles = store[owners, group, jnp.maximum(local, 0)]
            tiles = jnp.where((local >= 0)[:, None, None], tiles, jnp.zeros((), jnp.bfloat16))
            blocks.append(tiles.reshape(2, row_tiles, col_tiles, TR, TC))
        stacked = jnp.stack(blocks, axis=1)
        weight = stacked.transpose(0, 1, 2, 4, 3, 5).reshape(2, D, FF)
        hit = expert_ids == expert
        routed = jnp.any(hit, axis=1)
        factor = lax.optimization_barrier(jnp.sum(jnp.where(hit, weights.astype(jnp.float32), jnp.float32(0.0)), axis=1))
        order = jnp.cumsum(routed.astype(jnp.int32)).astype(jnp.int32) - 1
        target = jnp.where(routed, order, limit).astype(jnp.int32)
        index = jnp.zeros((limit,), jnp.int32).at[target].set(jnp.arange(count, dtype=jnp.int32), mode='drop')
        valid = jnp.zeros((limit,), jnp.float32).at[target].set(jnp.float32(1.0), mode='drop')
        rows = normed[index]
        pre = jnp.dot(rows, weight[0], preferred_element_type=jnp.float32)
        hidden = jax.nn.silu(pre).astype(jnp.bfloat16)
        out = lax.dot_general(hidden, weight[1], (((1,), (1,)), ((), ())), preferred_element_type=jnp.float32).astype(jnp.bfloat16)
        term = out.astype(jnp.float32) * (factor[index] * valid)[:, None]
        return (total.at[index].add(term), None)
    total, _ = lax.scan(one_expert, values, jnp.arange(EXPERTS, dtype=jnp.int32))
    layer_out = total.astype(jnp.bfloat16)
    stream = layer_out.astype(jnp.float32)
    renorm = lax.rsqrt(lax.optimization_barrier(jnp.mean(stream * stream, axis=1, keepdims=True)) + 1e-06)
    next_normed = (stream * renorm).astype(jnp.bfloat16)
    next_scores = jax.nn.sigmoid(jnp.dot(next_normed, next_router, preferred_element_type=jnp.float32))
    return (layer_out, next_scores)
```

```python
import functools

import jax
import jax.numpy as jnp
from jax import lax
from jax.experimental import pallas as pl
from jax.experimental.pallas import tpu as pltpu
from jax.sharding import PartitionSpec as P

MESH = pl.DeviceIdType.MESH
CAP = 2
LANES = 128


def place(side):
    e = lax.axis_index("ep")
    x = lax.axis_index("dp")
    y, z, c = e // (2 * side), (e // 2) % side, e % 2
    a = y + c * (z - y)
    b = z + c * (y - z)
    return x, y, z, c, a, b


def on_line(side, a, b, c):
    wide, narrow = 2 * side - c * (2 * side - 2), 2 + c * (2 * side - 2)
    return a * wide + b * narrow


def send(src, dst, send_sem, recv_sem, ep, dp):
    pltpu.make_async_remote_copy(
        src_ref=src,
        dst_ref=dst,
        send_sem=send_sem,
        recv_sem=recv_sem,
        device_id={"ep": ep, "dp": dp},
        device_id_type=MESH,
    ).start()


def wait_bytes(ref, sem):
    pltpu.make_async_copy(ref, ref, sem).wait()


def greet(ep, dp):
    pl.semaphore_signal(
        pltpu.get_barrier_semaphore(), inc=1, device_id={"ep": ep, "dp": dp}, device_id_type=MESH
    )


def each(count, body):
    def step(j, carry):
        body(j)
        return carry

    lax.fori_loop(0, count, step, 0)


def gather_kernel(
    side,
    dps,
    chunks,
    part,
    pay_ref,
    router_ref,
    rows_ref,
    comb_ref,
    routers_ref,
    got,
    send_sem,
    recv_sem,
    router_send,
    router_recv,
):
    x, y, z, c, a, b = place(side)
    line = side * dps
    mine = a * dps + x
    me = lax.axis_index("ep")

    def hello(j):
        k = (mine + 1 + j) % line
        greet(on_line(side, k // dps, b, c) + c, k % dps)

    each(line - 1, hello)
    pl.semaphore_wait(pltpu.get_barrier_semaphore(), line - 1)

    def out(j):
        k = (mine + 1 + j) % line
        send(
            pay_ref.at[k % dps, k // dps],
            got.at[mine],
            send_sem,
            recv_sem,
            on_line(side, k // dps, b, c) + c,
            k % dps,
        )

    each(line - 1, out)

    def router_out(j):
        send(router_ref, routers_ref.at[x], router_send, router_recv, me, (x + 1 + j) % dps)

    each(dps - 1, router_out)
    got[mine] = pay_ref[x, a]
    routers_ref[x] = router_ref[...]
    wait_bytes(got.at[pl.ds(0, line - 1)], recv_sem)

    tok = pay_ref.shape[2]
    blocks = line // chunks
    depth = blocks * tok
    experts = 2 * side
    width = experts * blocks * CAP
    q = lax.broadcasted_iota(jnp.int32, (width, LANES), 0)
    k = lax.broadcasted_iota(jnp.int32, (width, LANES), 1)
    pick_t = (k == (q // (blocks * CAP)) * CAP + q % CAP).astype(jnp.float32).astype(jnp.bfloat16)
    q = lax.broadcasted_iota(jnp.int32, (LANES, width), 1)
    k = lax.broadcasted_iota(jnp.int32, (LANES, width), 0)
    pick = (k == (q // (blocks * CAP)) * CAP + q % CAP).astype(jnp.float32).astype(jnp.bfloat16)
    r = lax.broadcasted_iota(jnp.int32, (depth, width), 0)
    q = lax.broadcasted_iota(jnp.int32, (depth, width), 1)
    own = r // tok == (q % (blocks * CAP)) // CAP
    r = lax.broadcasted_iota(jnp.int32, (width, depth), 1)
    q = lax.broadcasted_iota(jnp.int32, (width, depth), 0)
    own_t = r // tok == (q % (blocks * CAP)) // CAP
    for i in range(chunks):
        piece = got[i * blocks : (i + 1) * blocks].reshape(depth, part + LANES)
        comb = piece[:, part:]
        spread = jnp.dot(comb, pick, preferred_element_type=jnp.float32)
        comb_ref[i] = jnp.where(own, spread, 0.0).astype(jnp.bfloat16)
        spread_t = lax.dot_general(
            pick_t, comb, (((1,), (1,)), ((), ())), preferred_element_type=jnp.float32
        )
        named = jnp.where(own_t & (spread_t != 0.0), 1.0, 0.0).astype(jnp.bfloat16)
        rows = jnp.dot(named, piece[:, :part], preferred_element_type=jnp.float32)
        rows_ref[i] = rows.astype(jnp.bfloat16).reshape(experts, blocks * CAP, part)

    wait_bytes(routers_ref.at[pl.ds(0, dps - 1)], router_recv)
    wait_bytes(routers_ref.at[pl.ds(0, dps - 1)], router_send)
    wait_bytes(got.at[pl.ds(0, line - 1)], send_sem)


def layer_kernel(
    side,
    dps,
    chunks,
    rows_ref,
    comb_ref,
    tiles_hbm,
    map_ref,
    tokens_ref,
    routers_ref,
    out_ref,
    scores_ref,
    tiles,
    up,
    down,
    recv,
    pre,
    sums,
    hid,
    res,
    ret,
    mix,
    fin,
    tile_sem,
    row_send,
    row_recv,
    sum_send,
    sum_recv,
    hid_send,
    hid_recv,
    ret_send,
    ret_recv,
    fin_send,
    fin_recv,
):
    x, y, z, c, a, b = place(side)
    me = lax.axis_index("ep")
    line = side * dps
    mine = a * dps + x
    experts = 2 * side
    as_expert = b * 2 + c
    as_source = c * side + b
    part = up.shape[0]
    hidden = up.shape[1]
    slots = rows_ref.shape[2]
    tok = tokens_ref.shape[0]
    blocks = line // chunks

    tile_copy = pltpu.make_async_copy(tiles_hbm, tiles, tile_sem)
    tile_copy.start()

    def expert_at(d):
        return on_line(side, a, d // 2, c) + d % 2

    def source_at(s):
        other, i = s // side, s % side
        first = y * 2 * side + i * 2
        second = i * 2 * side + z * 2 + 1
        return first + other * (second - first)

    def line_at(k):
        return on_line(side, k // dps, b, c) + c

    def hello_experts(j):
        greet(expert_at((as_expert + 1 + j) % experts), x)

    def hello_sources(j):
        greet(source_at((as_source + 1 + j) % experts), x)

    def hello_line(j):
        k = (mine + 1 + j) % line
        greet(line_at(k), k % dps)

    each(experts - 1, hello_experts)
    each(experts - 1, hello_sources)
    each(line - 1, hello_line)
    pl.semaphore_wait(pltpu.get_barrier_semaphore(), 2 * (experts - 1) + line - 1)

    for i in range(chunks):

        def row_out(j, i=i):
            d = (as_expert + 1 + j) % experts
            send(
                rows_ref.at[i, d],
                recv.at[i, as_source],
                row_send.at[i],
                row_recv.at[i],
                expert_at(d),
                x,
            )

        each(experts - 1, row_out)
        recv[i, as_source] = rows_ref[i, as_expert]

    tile_copy.wait()
    row_tiles, col_tiles = part // LANES, hidden // LANES
    for m, weight in enumerate((up, down)):
        for r in range(row_tiles):
            for k in range(col_tiles):
                s = (m * row_tiles + r) * col_tiles + k
                weight[r * LANES : (r + 1) * LANES, k * LANES : (k + 1) * LANES] = tiles[
                    map_ref[0, s]
                ]

    def to_hidden(i):
        wait_bytes(recv.at[i, pl.ds(0, experts - 1)], row_recv.at[i])
        rows = recv[i].reshape(experts * slots, part)
        product = jnp.dot(rows, up[...], preferred_element_type=jnp.float32)
        pre[i] = product.astype(jnp.bfloat16).reshape(dps, experts * slots // dps, hidden)

        def out(j):
            other = (x + 1 + j) % dps
            send(pre.at[i, other], sums.at[i, x], sum_send.at[i], sum_recv.at[i], me, other)

        each(dps - 1, out)

    def activate(i):
        wait_bytes(sums.at[i, pl.ds(0, dps - 1)], sum_recv.at[i])
        total = pre[i, x].astype(jnp.float32)
        for j in range(1, dps):
            total = total + sums[i, (x + j) % dps].astype(jnp.float32)
        hid[i, x] = (total * jax.nn.sigmoid(total)).astype(jnp.bfloat16)

        def out(j):
            send(
                hid.at[i, x], hid.at[i, x], hid_send.at[i], hid_recv.at[i], me, (x + 1 + j) % dps
            )

        each(dps - 1, out)

    def to_result(i):
        wait_bytes(hid.at[i, pl.ds(0, dps - 1)], hid_recv.at[i])
        units = hid[i].reshape(experts * slots, hidden)
        product = lax.dot_general(
            units, down[...], (((1,), (1,)), ((), ())), preferred_element_type=jnp.float32
        )
        res[i] = product.astype(jnp.bfloat16).reshape(experts, slots, part)

        def out(j):
            s = (as_source + 1 + j) % experts
            other = s // side
            slot = (z + other * (y - z)) * 2 + c
            send(res.at[i, s], ret.at[i, slot], ret_send.at[i], ret_recv.at[i], source_at(s), x)

        each(experts - 1, out)
        ret[i, as_expert] = res[i, as_source]

    def combine(i):
        wait_bytes(ret.at[i, pl.ds(0, experts - 1)], ret_recv.at[i])
        outs = ret[i].reshape(experts * slots, part)
        mixed = jnp.dot(comb_ref[i], outs, preferred_element_type=jnp.float32)
        mix[pl.ds(i * blocks, blocks)] = mixed.astype(jnp.bfloat16).reshape(blocks, tok, part)

        def out(j):
            k = i * blocks + (j + x) % blocks

            @pl.when(k != mine)
            def _():
                send(mix.at[k], fin.at[mine], fin_send, fin_recv, line_at(k), k % dps)

        each(blocks, out)

    steps = (to_hidden, activate, to_result, combine)
    lag = (0, 1, 2, 4)
    for turn in range(chunks + lag[-1]):
        for step, late in zip(steps, lag):
            if 0 <= turn - late < chunks:
                step(turn - late)

    fin[mine] = mix[mine]
    wait_bytes(fin.at[pl.ds(0, line - 1)], fin_recv)
    squares = jnp.zeros((tok, 1), jnp.float32)
    for g in range(dps):
        total = fin[g].astype(jnp.float32)
        for other in range(1, side):
            total = total + fin[other * dps + g].astype(jnp.float32)
        columns = slice(g * part, (g + 1) * part)
        layer = (tokens_ref[:, columns].astype(jnp.float32) + total).astype(jnp.bfloat16)
        out_ref[:, columns] = layer
        stream = layer.astype(jnp.float32)
        squares = squares + jnp.sum(stream * stream, axis=1, keepdims=True)
    renorm = lax.rsqrt(squares / (dps * part) + 1e-06)
    logits = jnp.zeros((tok, scores_ref.shape[1]), jnp.float32)
    for g in range(dps):
        stream = out_ref[:, g * part : (g + 1) * part].astype(jnp.float32)
        normed = (stream * renorm).astype(jnp.bfloat16)
        logits = logits + jnp.dot(normed, routers_ref[g], preferred_element_type=jnp.float32)
    scores_ref[...] = jax.nn.sigmoid(logits)

    wait_bytes(fin.at[pl.ds(0, line - 1)], fin_send)
    for i in range(chunks):
        wait_bytes(recv.at[i, pl.ds(0, experts - 1)], row_send.at[i])
        wait_bytes(sums.at[i, pl.ds(0, dps - 1)], sum_send.at[i])
        wait_bytes(hid.at[i, pl.ds(0, dps - 1)], hid_send.at[i])
        wait_bytes(ret.at[i, pl.ds(0, experts - 1)], ret_send.at[i])


def vmem():
    return pl.BlockSpec(memory_space=pltpu.VMEM)


def per_device(side, tokens, norm_gain, router, next_router, expert_ids, store, send_list, cache_map):
    tok, width = tokens.shape
    dps = lax.axis_size("dp")
    experts = router.shape[1]
    top = expert_ids.shape[1]
    tiles = cache_map.shape[1]
    part = width // dps
    row_tiles = part // LANES
    hidden = tiles // (2 * row_tiles) * LANES
    line = side * dps
    chunks = 4 if side % 4 == 0 else 1
    slots = line // chunks * CAP
    bf16 = jnp.bfloat16

    owned = store.reshape(tiles, LANES, LANES)
    leaving = owned[jnp.maximum(send_list.reshape(-1), 0)]
    arrived = lax.all_to_all(leaving, "ep", split_axis=0, concat_axis=0, tiled=True)

    values = tokens.astype(jnp.float32)
    scale = lax.rsqrt(jnp.mean(values * values, axis=1, keepdims=True) + 1e-06)
    normed = (values * scale * norm_gain).astype(bf16)
    scores = jax.nn.sigmoid(jnp.dot(normed, router, preferred_element_type=jnp.float32))
    chosen = (expert_ids[:, :, None] == jnp.arange(experts, dtype=jnp.int32)).astype(jnp.float32)
    picked = jnp.sum(chosen * scores[:, None, :], axis=2)
    weights = (2.5 * picked / jnp.sum(picked, axis=1, keepdims=True)).astype(bf16)
    named = jnp.sum(chosen, axis=1)
    earlier = jnp.cumsum(named, axis=0) - named
    rank = jnp.sum(earlier[:, None, :] * chosen, axis=2).astype(jnp.int32)
    core = lax.axis_index("ep") % 2
    y, z, c = expert_ids // (2 * side), (expert_ids // 2) % side, expert_ids % 2
    turned = jnp.where(core == 1, z * (2 * side) + y * 2 + c, expert_ids)
    match = (turned * CAP + rank)[:, :, None] == jnp.arange(experts * CAP, dtype=jnp.int32)
    combine = jnp.sum(jnp.where(match, weights.astype(jnp.float32)[:, :, None], 0.0), axis=1)
    combine = combine.astype(bf16).reshape(tok, side, experts * CAP // side).transpose(1, 0, 2)
    combine = jnp.pad(combine, ((0, 0), (0, 0), (0, LANES - combine.shape[2])))
    pay = jnp.concatenate(
        [
            jnp.broadcast_to(
                normed.reshape(tok, dps, part).transpose(1, 0, 2)[:, None], (dps, side, tok, part)
            ),
            jnp.broadcast_to(combine[None], (dps, side, tok, LANES)),
        ],
        axis=3,
    )
    depth = line // chunks * tok
    rows, comb, routers = pl.pallas_call(
        functools.partial(gather_kernel, side, dps, chunks, part),
        out_shape=(
            jax.ShapeDtypeStruct((chunks, 2 * side, slots, part), bf16),
            jax.ShapeDtypeStruct((chunks, depth, 2 * side * slots), bf16),
            jax.ShapeDtypeStruct((dps, part, next_router.shape[1]), bf16),
        ),
        in_specs=[vmem()] * 2,
        out_specs=(vmem(),) * 3,
        scratch_shapes=[pltpu.VMEM((line, tok, part + LANES), bf16)]
        + [pltpu.SemaphoreType.DMA] * 4,
        compiler_params=pltpu.CompilerParams(
            collective_id=0, has_side_effects=True, vmem_limit_bytes=24 << 20
        ),
    )(pay, next_router)

    rows_all = 2 * side * slots
    shared = pltpu.VMEM((chunks, dps, rows_all // dps, hidden), bf16)
    traded = pltpu.VMEM((chunks, 2 * side, slots, part), bf16)
    lined = pltpu.VMEM((line, tok, part), bf16)
    dma = pltpu.SemaphoreType.DMA((chunks,))
    return pl.pallas_call(
        functools.partial(layer_kernel, side, dps, chunks),
        out_shape=(
            jax.ShapeDtypeStruct((tok, width), bf16),
            jax.ShapeDtypeStruct((tok, next_router.shape[1]), jnp.float32),
        ),
        in_specs=[
            vmem(),
            vmem(),
            pl.BlockSpec(memory_space=pl.ANY),
            pl.BlockSpec(memory_space=pltpu.SMEM),
            vmem(),
            vmem(),
        ],
        out_specs=(vmem(), vmem()),
        scratch_shapes=[
            pltpu.VMEM(arrived.shape, bf16),
            pltpu.VMEM((part, hidden), bf16),
            pltpu.VMEM((part, hidden), bf16),
            traded,
            shared,
            shared,
            shared,
            traded,
            traded,
            lined,
            lined,
            pltpu.SemaphoreType.DMA,
        ]
        + [dma] * 8
        + [pltpu.SemaphoreType.DMA] * 2,
        compiler_params=pltpu.CompilerParams(
            collective_id=1, has_side_effects=True, vmem_limit_bytes=56 << 20
        ),
    )(rows, comb, arrived, cache_map, tokens, routers)


def solution(mesh):
    side = round((mesh.shape["ep"] // 2) ** 0.5)
    in_specs = (
        P(("ep", "dp"), None),
        P(),
        P(),
        P("dp", None),
        P(("ep", "dp"), None),
        P("ep", "dp", None, None, None),
        P("ep", None),
        P("ep", None),
    )
    out_specs = (P(("ep", "dp"), None), P(("ep", "dp"), None))
    return jax.shard_map(
        functools.partial(per_device, side),
        mesh=mesh,
        in_specs=in_specs,
        out_specs=out_specs,
        check_vma=False,
    )
```

```python
import functools

import jax
import jax.numpy as jnp
from jax import lax
from jax.experimental import pallas as pl
from jax.experimental.pallas import tpu as pltpu
from jax.sharding import PartitionSpec as P

MESH = pl.DeviceIdType.MESH
CAP = 2
LANES = 128
LAG = (0, 1, 2, 3, 4, 6)
ORDER = -1


def place(side):
    e = lax.axis_index("ep")
    x = lax.axis_index("dp")
    y, z, c = e // (2 * side), (e // 2) % side, e % 2
    a = y + c * (z - y)
    b = z + c * (y - z)
    return x, y, z, c, a, b


def on_line(side, a, b, c):
    wide, narrow = 2 * side - c * (2 * side - 2), 2 + c * (2 * side - 2)
    return a * wide + b * narrow


def send(src, dst, send_sem, recv_sem, ep, dp):
    pltpu.make_async_remote_copy(
        src_ref=src,
        dst_ref=dst,
        send_sem=send_sem,
        recv_sem=recv_sem,
        device_id={"ep": ep, "dp": dp},
        device_id_type=MESH,
    ).start()


def wait_bytes(ref, sem):
    pltpu.make_async_copy(ref, ref, sem).wait()


def greet(ep, dp):
    pl.semaphore_signal(
        pltpu.get_barrier_semaphore(), inc=1, device_id={"ep": ep, "dp": dp}, device_id_type=MESH
    )


def each(count, body):
    def step(j, carry):
        body(j)
        return carry

    lax.fori_loop(0, count, step, 0)


def layer_kernel(
    side,
    dps,
    chunks,
    pay_ref,
    router_ref,
    store_hbm,
    list_ref,
    map_ref,
    tokens_ref,
    out_ref,
    scores_ref,
    store,
    leave,
    mid,
    arrived,
    up,
    down,
    got,
    rows_out,
    comb_all,
    routers,
    recv,
    pre,
    half,
    sums,
    hid,
    res,
    ret,
    mix,
    fin,
    store_sem,
    got_send,
    got_recv,
    router_send,
    router_recv,
    leave_send,
    mid_recv,
    tile_send,
    tile_recv,
    row_send,
    row_recv,
    half_send,
    half_recv,
    sum_send,
    sum_recv,
    hid_send,
    hid_recv,
    pass_send,
    pass_recv,
    ret_send,
    ret_recv,
    fin_send,
    fin_recv,
):
    x, y, z, c, a, b = place(side)
    me = lax.axis_index("ep")
    line = side * dps
    mine = a * dps + x
    experts = 2 * side
    as_expert = b * 2 + c
    as_source = c * side + b
    part, hidden = up.shape
    slots = recv.shape[2]
    tok = tokens_ref.shape[0]
    blocks = line // chunks
    right, left, far = (x + 1) % dps, (x + dps - 1) % dps, (x + 2) % dps

    store_copy = pltpu.make_async_copy(store_hbm, store, store_sem)
    store_copy.start()

    def expert_at(d):
        return on_line(side, a, d // 2, c) + d % 2

    def source_at(s):
        other, i = s // side, s % side
        first = y * 2 * side + i * 2
        second = i * 2 * side + z * 2 + 1
        return first + other * (second - first)

    def line_at(k):
        return on_line(side, k // dps, b, c) + c

    def hello_experts(j):
        greet(expert_at((as_expert + 1 + j) % experts), x)

    def hello_sources(j):
        greet(source_at((as_source + 1 + j) % experts), x)

    def hello_line(j):
        k = (mine + 1 + j) % line
        greet(line_at(k), k % dps)

    each(experts - 1, hello_experts)
    each(experts - 1, hello_sources)
    each(line - 1, hello_line)
    pl.semaphore_wait(pltpu.get_barrier_semaphore(), 2 * (experts - 1) + line - 1)

    def token_out(j):
        k = (mine + 1 + j) % line
        send(pay_ref.at[k % dps, k // dps], got.at[mine], got_send, got_recv, line_at(k), k % dps)

    each(line - 1, token_out)

    steps_b = [(d, (side - d) % side) for d in range(side // 2 - 1, 0, -1)]
    steps_b.insert(1 if side > 2 else 0, (side // 2, 0))
    store_copy.wait()
    for i in range(chunks):

        def pick(j, i=i):
            there = (a + 1 + j) % side
            for q in range(4):
                ep = on_line(side, there, (b + steps_b[i][q // 2]) % side, c) + q % 2
                leave[i, j, q] = store[jnp.maximum(list_ref[0, ep], 0)]

        each(side, pick)

        def tile_out(j, i=i):
            there = (a + 1 + j) % side
            send(
                leave.at[i, j],
                mid.at[i, a],
                leave_send.at[i],
                mid_recv.at[i],
                on_line(side, there, b, c) + c,
                x,
            )

        each(side - 1, tile_out)
        mid[i, a] = leave[i, side - 1]

    def router_out(j):
        send(router_ref, routers.at[x], router_send, router_recv, me, (x + 1 + j) % dps)

    each(dps - 1, router_out)
    got[mine] = pay_ref[x, a]
    routers[x] = router_ref[...]

    depth = blocks * tok
    width = experts * slots
    q = lax.broadcasted_iota(jnp.int32, (width, LANES), 0)
    k = lax.broadcasted_iota(jnp.int32, (width, LANES), 1)
    pick_t = (k == (q // slots) * CAP + q % CAP).astype(jnp.float32).astype(jnp.bfloat16)
    q = lax.broadcasted_iota(jnp.int32, (LANES, width), 1)
    k = lax.broadcasted_iota(jnp.int32, (LANES, width), 0)
    pick_n = (k == (q // slots) * CAP + q % CAP).astype(jnp.float32).astype(jnp.bfloat16)
    r = lax.broadcasted_iota(jnp.int32, (depth, width), 0)
    q = lax.broadcasted_iota(jnp.int32, (depth, width), 1)
    own = r // tok == (q % slots) // CAP
    r = lax.broadcasted_iota(jnp.int32, (width, depth), 1)
    q = lax.broadcasted_iota(jnp.int32, (width, depth), 0)
    own_t = r // tok == (q % slots) // CAP
    wait_bytes(got.at[pl.ds(0, line - 1)], got_recv)
    for i in range(chunks):
        piece = got[i * blocks : (i + 1) * blocks].reshape(depth, part + LANES)
        comb = piece[:, part:]
        spread = jnp.dot(comb, pick_n, preferred_element_type=jnp.float32)
        comb_all[i] = jnp.where(own, spread, 0.0).astype(jnp.bfloat16)
        spread_t = lax.dot_general(
            pick_t, comb, (((1,), (1,)), ((), ())), preferred_element_type=jnp.float32
        )
        named = jnp.where(own_t & (spread_t != 0.0), 1.0, 0.0).astype(jnp.bfloat16)
        rows = jnp.dot(named, piece[:, :part], preferred_element_type=jnp.float32)
        rows_out[i] = rows.astype(jnp.bfloat16).reshape(experts, slots, part)

    def rows_away(i):
        def out(j):
            d = (as_expert + 1 + j) % experts
            send(
                rows_out.at[i, d],
                recv.at[i, as_source],
                row_send.at[i],
                row_recv.at[i],
                expert_at(d),
                x,
            )

        each(experts - 1, out)
        recv[i, as_source] = rows_out[i, as_expert]

    for i in range(chunks):
        wait_bytes(mid.at[i, pl.ds(0, side - 1)], mid_recv.at[i])
        if i == chunks - 1:
            rows_away(0)
        for q in range(4):
            ahead = steps_b[i][q // 2]
            ep = on_line(side, a, (b + ahead) % side, c) + q % 2

            def tile_on(i=i, q=q, ep=ep):
                send(mid.at[i, :, q], arrived.at[as_source], tile_send, tile_recv, ep, x)

            if ahead:
                tile_on()
            else:
                pl.when(c != q % 2)(tile_on)

                @pl.when(c == q % 2)
                def _(i=i, q=q):
                    arrived[as_source] = mid[i, :, q]

    for i in range(1, chunks):
        rows_away(i)

    wait_bytes(arrived.at[pl.ds(0, experts - 1)], tile_recv)
    row_tiles, col_tiles = part // LANES, hidden // LANES
    for m, weight in enumerate((up, down)):

        def assemble(r, m=m, weight=weight):
            for k in range(col_tiles):
                n = map_ref[0, (m * row_tiles + r) * col_tiles + k]
                yn, zn, cn = n // (2 * side), (n // 2) % side, n % 2
                along = cn * (zn - yn)
                tile = arrived[cn * side + zn - along, yn + along]
                weight[pl.ds(pl.multiple_of(r * LANES, LANES), LANES), pl.ds(k * LANES, LANES)] = (
                    tile
                )

        each(row_tiles, assemble)

    rows_each = experts * slots // dps
    cut = rows_each // 2

    def to_hidden(i):
        wait_bytes(recv.at[i, pl.ds(0, experts - 1)], row_recv.at[i])
        rows = recv[i].reshape(experts * slots, part)
        product = jnp.dot(rows, up[...], preferred_element_type=jnp.float32)
        pre[i] = product.astype(jnp.bfloat16).reshape(dps, rows_each, hidden)
        top, low = pl.ds(0, cut), pl.ds(cut, cut)
        send(pre.at[i, far, top], half.at[i, 0], half_send.at[i], half_recv.at[i], me, right)
        send(pre.at[i, far, low], half.at[i, 1], half_send.at[i], half_recv.at[i], me, left)

    def relay(i):
        wait_bytes(half.at[i], half_recv.at[i])
        for k, (other, start) in enumerate(((right, 0), (left, cut))):
            piece = pl.ds(start, cut)
            total = pre[i, other, piece].astype(jnp.float32) + half[i, k].astype(jnp.float32)
            pre[i, other, piece] = total.astype(jnp.bfloat16)
            send(pre.at[i, other], sums.at[i, k], sum_send.at[i], sum_recv.at[i], me, other)

    def activate(i):
        wait_bytes(sums.at[i], sum_recv.at[i])
        total = pre[i, x].astype(jnp.float32)
        total = total + sums[i, 0].astype(jnp.float32) + sums[i, 1].astype(jnp.float32)
        hid[i, x] = (total * jax.nn.sigmoid(total)).astype(jnp.bfloat16)
        for other in (right, left):
            send(hid.at[i, x], hid.at[i, x], hid_send.at[i], hid_recv.at[i], me, other)

    def pass_on(i):
        wait_bytes(sums.at[i], hid_recv.at[i])
        for other, source, start in ((right, left, 0), (left, right, cut)):
            piece = hid.at[i, source, pl.ds(start, cut)]
            send(piece, piece, pass_send.at[i], pass_recv.at[i], me, other)

    def to_result(i):
        wait_bytes(half.at[i], pass_recv.at[i])
        units = hid[i].reshape(experts * slots, hidden)
        product = lax.dot_general(
            units, down[...], (((1,), (1,)), ((), ())), preferred_element_type=jnp.float32
        )
        res[i] = product.astype(jnp.bfloat16).reshape(experts, slots, part)

        def out(j):
            s = (as_source + 1 + j) % experts
            other = s // side
            slot = (z + other * (y - z)) * 2 + c
            send(res.at[i, s], ret.at[i, slot], ret_send.at[i], ret_recv.at[i], source_at(s), x)

        each(experts - 1, out)
        ret[i, as_expert] = res[i, as_source]

    def combine(i):
        wait_bytes(ret.at[i, pl.ds(0, experts - 1)], ret_recv.at[i])
        outs = ret[i].reshape(experts * slots, part)
        mixed = jnp.dot(comb_all[i], outs, preferred_element_type=jnp.float32)
        mix[pl.ds(i * blocks, blocks)] = mixed.astype(jnp.bfloat16).reshape(blocks, tok, part)

        def out(j):
            k = i * blocks + (j + x) % blocks

            @pl.when(k != mine)
            def _():
                send(mix.at[k], fin.at[mine], fin_send, fin_recv, line_at(k), k % dps)

        each(blocks, out)

    steps = (to_hidden, relay, activate, pass_on, to_result, combine)
    for turn in range(chunks + LAG[-1]):
        for step, late in sorted(zip(steps, LAG), key=lambda p: ORDER * p[1]):
            if 0 <= turn - late < chunks:
                step(turn - late)

    fin[mine] = mix[mine]
    wait_bytes(routers.at[pl.ds(0, dps - 1)], router_recv)
    wait_bytes(fin.at[pl.ds(0, line - 1)], fin_recv)
    squares = jnp.zeros((tok, 1), jnp.float32)
    for g in range(dps):
        total = fin[g].astype(jnp.float32)
        for other in range(1, side):
            total = total + fin[other * dps + g].astype(jnp.float32)
        columns = slice(g * part, (g + 1) * part)
        layer = (tokens_ref[:, columns].astype(jnp.float32) + total).astype(jnp.bfloat16)
        out_ref[:, columns] = layer
        stream = layer.astype(jnp.float32)
        squares = squares + jnp.sum(stream * stream, axis=1, keepdims=True)
    renorm = lax.rsqrt(squares / (dps * part) + 1e-06)
    logits = jnp.zeros((tok, scores_ref.shape[1]), jnp.float32)
    for g in range(dps):
        stream = out_ref[:, g * part : (g + 1) * part].astype(jnp.float32)
        normed = (stream * renorm).astype(jnp.bfloat16)
        logits = logits + jnp.dot(normed, routers[g], preferred_element_type=jnp.float32)
    scores_ref[...] = jax.nn.sigmoid(logits)

    wait_bytes(got.at[pl.ds(0, line - 1)], got_send)
    wait_bytes(routers.at[pl.ds(0, dps - 1)], router_send)
    wait_bytes(arrived.at[pl.ds(0, experts - 1)], tile_send)
    wait_bytes(fin.at[pl.ds(0, line - 1)], fin_send)
    for i in range(chunks):
        wait_bytes(mid.at[i, pl.ds(0, side - 1)], leave_send.at[i])
        wait_bytes(recv.at[i, pl.ds(0, experts - 1)], row_send.at[i])
        wait_bytes(half.at[i], half_send.at[i])
        wait_bytes(sums.at[i], sum_send.at[i])
        wait_bytes(sums.at[i], hid_send.at[i])
        wait_bytes(half.at[i], pass_send.at[i])
        wait_bytes(ret.at[i, pl.ds(0, experts - 1)], ret_send.at[i])


def vmem():
    return pl.BlockSpec(memory_space=pltpu.VMEM)


def per_device(side, tokens, norm_gain, router, next_router, expert_ids, store, send_list, cache_map):
    tok, width = tokens.shape
    dps = lax.axis_size("dp")
    experts = router.shape[1]
    top = expert_ids.shape[1]
    tiles = cache_map.shape[1]
    part = width // dps
    row_tiles = part // LANES
    hidden = tiles // (2 * row_tiles) * LANES
    line = side * dps
    chunks = side // 2
    slots = line // chunks * CAP
    bf16 = jnp.bfloat16

    values = tokens.astype(jnp.float32)
    scale = lax.rsqrt(jnp.mean(values * values, axis=1, keepdims=True) + 1e-06)
    normed = (values * scale * norm_gain).astype(bf16)
    scores = jax.nn.sigmoid(jnp.dot(normed, router, preferred_element_type=jnp.float32))
    chosen = (expert_ids[:, :, None] == jnp.arange(experts, dtype=jnp.int32)).astype(jnp.float32)
    picked = jnp.sum(chosen * scores[:, None, :], axis=2)
    weights = (2.5 * picked / jnp.sum(picked, axis=1, keepdims=True)).astype(bf16)
    named = jnp.sum(chosen, axis=1)
    earlier = jnp.cumsum(named, axis=0) - named
    rank = jnp.sum(earlier[:, None, :] * chosen, axis=2).astype(jnp.int32)
    core = lax.axis_index("ep") % 2
    y, z, c = expert_ids // (2 * side), (expert_ids // 2) % side, expert_ids % 2
    turned = jnp.where(core == 1, z * (2 * side) + y * 2 + c, expert_ids)
    match = (turned * CAP + rank)[:, :, None] == jnp.arange(experts * CAP, dtype=jnp.int32)
    combine = jnp.sum(jnp.where(match, weights.astype(jnp.float32)[:, :, None], 0.0), axis=1)
    combine = combine.astype(bf16).reshape(tok, side, experts * CAP // side).transpose(1, 0, 2)
    combine = jnp.pad(combine, ((0, 0), (0, 0), (0, LANES - combine.shape[2])))
    pay = jnp.concatenate(
        [
            jnp.broadcast_to(
                normed.reshape(tok, dps, part).transpose(1, 0, 2)[:, None], (dps, side, tok, part)
            ),
            jnp.broadcast_to(combine[None], (dps, side, tok, LANES)),
        ],
        axis=3,
    )
    rows_all = 2 * side * slots
    shared = pltpu.VMEM((chunks, dps, rows_all // dps, hidden), bf16)
    paired = pltpu.VMEM((chunks, 2, rows_all // dps, hidden), bf16)
    halves = pltpu.VMEM((chunks, 2, rows_all // dps // 2, hidden), bf16)
    traded = pltpu.VMEM((chunks, 2 * side, slots, part), bf16)
    lined = pltpu.VMEM((line, tok, part), bf16)
    weight = pltpu.VMEM((part, hidden), bf16)
    moved = pltpu.VMEM((chunks, side, 4, LANES, LANES), bf16)
    one = pltpu.SemaphoreType.DMA
    many = pltpu.SemaphoreType.DMA((chunks,))
    return pl.pallas_call(
        functools.partial(layer_kernel, side, dps, chunks),
        out_shape=(
            jax.ShapeDtypeStruct((tok, width), bf16),
            jax.ShapeDtypeStruct((tok, next_router.shape[1]), jnp.float32),
        ),
        in_specs=[
            vmem(),
            vmem(),
            pl.BlockSpec(memory_space=pl.ANY),
            pl.BlockSpec(memory_space=pltpu.SMEM),
            pl.BlockSpec(memory_space=pltpu.SMEM),
            vmem(),
        ],
        out_specs=(vmem(), vmem()),
        scratch_shapes=[
            pltpu.VMEM((tiles, LANES, LANES), bf16),
            moved,
            moved,
            pltpu.VMEM((2 * side, side, LANES, LANES), bf16),
            weight,
            weight,
            pltpu.VMEM((line, tok, part + LANES), bf16),
            traded,
            pltpu.VMEM((chunks, line // chunks * tok, rows_all), bf16),
            pltpu.VMEM((dps, part, next_router.shape[1]), bf16),
            traded,
            shared,
            halves,
            paired,
            shared,
            traded,
            traded,
            lined,
            lined,
        ]
        + [one] * 5
        + [many] * 2
        + [one] * 2
        + [many] * 12
        + [one] * 2,
        compiler_params=pltpu.CompilerParams(
            collective_id=0, has_side_effects=True, vmem_limit_bytes=58 << 20
        ),
    )(pay, next_router, store.reshape(tiles, LANES, LANES), send_list, cache_map, tokens)


def solution(mesh):
    side = round((mesh.shape["ep"] // 2) ** 0.5)
    in_specs = (
        P(("ep", "dp"), None),
        P(),
        P(),
        P("dp", None),
        P(("ep", "dp"), None),
        P("ep", "dp", None, None, None),
        P("ep", None),
        P("ep", None),
    )
    out_specs = (P(("ep", "dp"), None), P(("ep", "dp"), None))
    return jax.shard_map(
        functools.partial(per_device, side),
        mesh=mesh,
        in_specs=in_specs,
        out_specs=out_specs,
        check_vma=False,
    )
```

```python
import functools
import types

import jax
import jax.numpy as jnp
from jax import lax
from jax.experimental import pallas as pl
from jax.experimental.pallas import tpu as pltpu
from jax.sharding import PartitionSpec as P

MESH = pl.DeviceIdType.MESH
CAP = 2
LANES = 128
PIECES = 4
LAG = (0, 1, 2, 3, 4, 9)
ORDER = -1


def place(side):
    e = lax.axis_index("ep")
    x = lax.axis_index("dp")
    y, z, c = e // (2 * side), (e // 2) % side, e % 2
    a = y + c * (z - y)
    b = z + c * (y - z)
    return x, y, z, c, a, b


def on_line(side, a, b, c):
    wide, narrow = 2 * side - c * (2 * side - 2), 2 + c * (2 * side - 2)
    return a * wide + b * narrow


def send(src, dst, send_sem, recv_sem, ep, dp):
    pltpu.make_async_remote_copy(
        src_ref=src,
        dst_ref=dst,
        send_sem=send_sem,
        recv_sem=recv_sem,
        device_id={"ep": ep, "dp": dp},
        device_id_type=MESH,
    ).start()


def wait_bytes(ref, sem):
    pltpu.make_async_copy(ref, ref, sem).wait()


def greet(ep, dp):
    pl.semaphore_signal(
        pltpu.get_barrier_semaphore(), inc=1, device_id={"ep": ep, "dp": dp}, device_id_type=MESH
    )


def each(count, body):
    def step(j, carry):
        body(j)
        return carry

    lax.fori_loop(0, count, step, 0)


def hops_along(side):
    pairs = [(d, (side - d) % side) for d in range(side // 2 - 1, 0, -1)]
    pairs.insert(1 if side > 2 else 0, (side // 2, 0))
    return pairs


def layer_kernel(
    side,
    dps,
    chunks,
    names,
    tokens_ref,
    gain_ref,
    router_ref,
    next_ref,
    ids_ref,
    list_ref,
    map_ref,
    store_hbm,
    out_ref,
    scores_ref,
    *scratch,
):
    own_refs = types.SimpleNamespace(**dict(zip(names, scratch)))
    pay = own_refs.pay
    (store, mid, arrived, up, down, got, rows_out, comb_all, routers, recv) = scratch[:10]
    (pre, half, sums, hid, res, ret, mix, fin) = scratch[10:18]
    (store_sem, gx_send, gx_recv, router_send, router_recv, tile_send, tile_recv) = scratch[18:25]
    (fin_send, fin_recv, row_send, row_recv, half_send, half_recv) = scratch[25:31]
    (sum_send, sum_recv, hid_send, hid_recv, pass_send, pass_recv) = scratch[31:37]
    (ret_send, ret_recv, ag_send, ag_recv, along_send, along_recv) = scratch[37:43]
    (over_send, over_recv) = scratch[43:45]
    x, y, z, c, a, b = place(side)
    me = lax.axis_index("ep")
    line = side * dps
    mine = a * dps + x
    experts = 2 * side
    as_expert = b * 2 + c
    as_source = c * side + b
    part, hidden = up.shape
    slots = recv.shape[2]
    tok = tokens_ref.shape[0]
    blocks = line // chunks
    last = side // 2
    ways = ((0, 1), (1, side - 1))
    right, left, far = (x + 1) % dps, (x + dps - 1) % dps, (x + 2) % dps

    store_copy = pltpu.make_async_copy(store_hbm, store, store_sem)
    store_copy.start()

    def expert_at(d):
        return on_line(side, a, d // 2, c) + d % 2

    def source_at(s):
        other, i = s // side, s % side
        first = y * 2 * side + i * 2
        second = i * 2 * side + z * 2 + 1
        return first + other * (second - first)

    def line_at(k):
        return on_line(side, k // dps, b, c) + c

    def hello_experts(j):
        greet(expert_at((as_expert + 1 + j) % experts), x)

    def hello_sources(j):
        greet(source_at((as_source + 1 + j) % experts), x)

    def hello_line(j):
        k = (mine + 1 + j) % line
        greet(line_at(k), k % dps)

    each(experts - 1, hello_experts)
    each(experts - 1, hello_sources)
    each(line - 1, hello_line)
    pl.semaphore_wait(pltpu.get_barrier_semaphore(), 2 * (experts - 1) + line - 1)

    def route():
        values = tokens_ref[...].astype(jnp.float32)
        scale = lax.rsqrt(jnp.mean(values * values, axis=1, keepdims=True) + 1e-06)
        normed = (values * scale * gain_ref[...]).astype(jnp.bfloat16)
        logits = jnp.dot(normed, router_ref[...], preferred_element_type=jnp.float32)
        scores = jax.nn.sigmoid(logits)
        count = scores.shape[1]
        top = ids_ref.shape[0]
        ids = lax.dot_general(
            (
                lax.broadcasted_iota(jnp.int32, (tok, tok), 0)
                == lax.broadcasted_iota(jnp.int32, (tok, tok), 1)
            ).astype(jnp.float32),
            ids_ref[...].astype(jnp.float32),
            (((1,), (1,)), ((), ())),
            preferred_element_type=jnp.float32,
        ).astype(jnp.int32)
        lane = lax.broadcasted_iota(jnp.int32, (tok, count), 1)
        hits = [(ids[:, k : k + 1] == lane).astype(jnp.float32) for k in range(top)]
        picked = [jnp.sum(hit * scores, axis=1, keepdims=True) for hit in hits]
        total = functools.reduce(jnp.add, picked)
        weights = [(2.5 * p / total).astype(jnp.bfloat16).astype(jnp.float32) for p in picked]
        weight = functools.reduce(jnp.add, [hit * w for hit, w in zip(hits, weights)])
        named = functools.reduce(jnp.add, hits)
        earlier = (
            lax.broadcasted_iota(jnp.int32, (tok, tok), 0)
            > lax.broadcasted_iota(jnp.int32, (tok, tok), 1)
        ).astype(jnp.float32)
        rank = jnp.dot(earlier, named, preferred_element_type=jnp.float32)
        lanes = pay.shape[2] - part
        e = lax.broadcasted_iota(jnp.int32, (count, lanes), 0)
        column = lax.broadcasted_iota(jnp.int32, (count, lanes), 1)
        ye, ze, ce = e // (2 * side), (e // 2) % side, e % 2
        turn_y, turn_z = ye + c * (ze - ye), ze + c * (ye - ze)
        first = (turn_y * (2 * side) + turn_z * 2 + ce) * CAP
        combine = jnp.zeros((tok, lanes), jnp.float32)
        for r in range(CAP):
            ranked = jnp.where(rank == r, weight, 0.0).astype(jnp.bfloat16)
            place_r = (column == first + r).astype(jnp.float32).astype(jnp.bfloat16)
            combine = combine + jnp.dot(ranked, place_r, preferred_element_type=jnp.float32)
        for g in range(dps):
            pay[g, :, :part] = normed[:, g * part : (g + 1) * part]
            pay[g, :, part:] = combine.astype(jnp.bfloat16)

    def tokens_out():
        def out(j):
            other = (x + 1 + j) % dps
            send(pay.at[other], got.at[a, x], gx_send, gx_recv, me, other)

        each(dps - 1, out)
        got[a, x] = pay[x]

    def tokens_step(k):
        if k == 0:
            wait_bytes(got.at[a, pl.ds(0, dps - 1)], gx_recv)
        else:
            for d, step in ways:
                block = got.at[0] if k < last else got.at[0, pl.ds(0, dps // 2)]
                wait_bytes(block, ag_recv.at[d, k - 1])
        if k == last:
            return
        for d, step in ways:
            origin = (a + side - k if d == 0 else a + k) % side
            block = got.at[origin]
            if k + 1 == last:
                block = got.at[origin, pl.ds(d * (dps // 2), dps // 2)]
            to = on_line(side, (a + step) % side, b, c) + c
            send(block, block, ag_send.at[d, k], ag_recv.at[d, k], to, x)

    pairs = hops_along(side)
    outs, ins = own_refs.out1, [None] + [getattr(own_refs, f"in{k}") for k in range(1, last + 1)]

    def tile_for(i, q, h, there):
        ep = on_line(side, there, (b + pairs[i][q]) % side, c) + h
        return store[jnp.maximum(list_ref[0, ep], 0)]

    def along_start(i):
        for d, step in ways:

            def near(j, d=d):
                there = (a + 1 + j if d == 0 else a + side - 1 - j) % side
                for h in range(2):
                    for q in range(2):
                        outs[d, i, 2 * j + h, q] = tile_for(i, q, h, there)

            if last > 1:
                each(last - 1, near)
            for q in range(2):
                outs[d, i, 2 * (last - 1), q] = tile_for(i, q, d, (a + last) % side)
            to = on_line(side, (a + step) % side, b, c) + c
            send(outs.at[d, i], ins[1].at[d, i], along_send.at[d, i, 0], along_recv.at[d, i, 0], to, x)
        for h in range(2):
            for q in range(2):
                mid[i, q, h, a] = tile_for(i, q, h, a)

    def along_step(i, k):
        for d, step in ways:
            wait_bytes(ins[k].at[d, i], along_recv.at[d, i, k - 1])
            if k < last:
                rest = ins[k].at[d, i, pl.ds(2, side - 1 - 2 * k)]
                to = on_line(side, (a + step) % side, b, c) + c
                send(
                    rest, ins[k + 1].at[d, i], along_send.at[d, i, k], along_recv.at[d, i, k], to, x
                )
        for d, step in ways:
            origin = (a + side - k if d == 0 else a + k) % side
            for h in (0, 1) if k < last else (d,):
                for q in range(2):
                    mid[i, q, h, origin] = ins[k][d, i, h if k < last else 0, q]

    def over_hops(i):
        return min(pairs[i][0], side - pairs[i][0])

    def over_step(i, k):
        hops = over_hops(i)
        split = hops == last
        trail = getattr(own_refs, f"over{i}")
        for d, step in ways:
            if k == 1:
                block = mid.at[i, 0, d] if split else mid.at[i, d]
            else:
                block = trail.at[k - 2, d]
                wait_bytes(block, over_recv.at[d, i, k - 2])
            to = on_line(side, a, (b + step) % side, c)
            origin = c * side + (b + side - k + 1 if d == 0 else b + k - 1) % side
            if k < hops:
                sems = over_send.at[d, i, k - 1], over_recv.at[d, i, k - 1]
                send(block, trail.at[k - 1, d], *sems, to + c, x)
            elif split:
                send(block, arrived.at[origin], tile_send, tile_recv, to + d, x)
            else:
                for h in range(2):
                    send(block.at[h], arrived.at[origin], tile_send, tile_recv, to + h, x)
        if split and k == 1:
            pair = me + 1 - 2 * c
            send(mid.at[i, 1, 1 - c], arrived.at[as_source], tile_send, tile_recv, pair, x)
            arrived[as_source] = mid[i, 1, c]

    def build_rows():
        depth = blocks * tok
        width = experts * slots
        lanes = got.shape[3] - part
        first = a * experts * CAP
        q = lax.broadcasted_iota(jnp.int32, (width, lanes), 0)
        k = lax.broadcasted_iota(jnp.int32, (width, lanes), 1)
        pick_t = (k == first + (q // slots) * CAP + q % CAP).astype(jnp.float32).astype(jnp.bfloat16)
        q = lax.broadcasted_iota(jnp.int32, (lanes, width), 1)
        k = lax.broadcasted_iota(jnp.int32, (lanes, width), 0)
        pick_n = (k == first + (q // slots) * CAP + q % CAP).astype(jnp.float32).astype(jnp.bfloat16)
        r = lax.broadcasted_iota(jnp.int32, (depth, width), 0)
        q = lax.broadcasted_iota(jnp.int32, (depth, width), 1)
        own = r // tok == (q % slots) // CAP
        r = lax.broadcasted_iota(jnp.int32, (width, depth), 1)
        q = lax.broadcasted_iota(jnp.int32, (width, depth), 0)
        own_t = r // tok == (q % slots) // CAP
        lines = got.shape[0] // chunks
        for i in range(chunks):
            piece = got[i * lines : (i + 1) * lines].reshape(depth, part + lanes)
            comb = piece[:, part:]
            spread = jnp.dot(comb, pick_n, preferred_element_type=jnp.float32)
            comb_all[i] = jnp.where(own, spread, 0.0).astype(jnp.bfloat16)
            spread_t = lax.dot_general(
                pick_t, comb, (((1,), (1,)), ((), ())), preferred_element_type=jnp.float32
            )
            named = jnp.where(own_t & (spread_t != 0.0), 1.0, 0.0).astype(jnp.bfloat16)
            rows = jnp.dot(named, piece[:, :part], preferred_element_type=jnp.float32)
            rows_out[i] = rows.astype(jnp.bfloat16).reshape(experts, slots, part)

    def rows_away(i):
        def out(j):
            d = (as_expert + 1 + j) % experts
            send(
                rows_out.at[i, d],
                recv.at[i, as_source],
                row_send.at[i],
                row_recv.at[i],
                expert_at(d),
                x,
            )

        each(experts - 1, out)
        recv[i, as_source] = rows_out[i, as_expert]

    def router_out(j):
        send(next_ref, routers.at[x], router_send, router_recv, me, (x + 1 + j) % dps)

    store_copy.wait()
    loads = len(pairs)
    late = min(1, loads - 1)
    for turn in range(loads + 2 * last):
        if turn < loads:
            along_start(turn)
        if turn == 0:
            route()
            tokens_out()
            each(dps - 1, router_out)
            routers[x] = next_ref[...]
        if late <= turn <= last + late:
            tokens_step(turn - late)
        for k in range(1, last + 1):
            if 0 <= turn - k < loads:
                along_step(turn - k, k)
        if turn == last + late:
            build_rows()
        for k in range(1, last + 1):
            i = turn - last - k + 1
            if 0 <= i < loads and k <= over_hops(i):
                if k == 1 and i == loads - 1:
                    rows_away(0)
                over_step(i, k)

    for i in range(1, chunks):
        rows_away(i)

    wait_bytes(arrived.at[pl.ds(0, experts - 1)], tile_recv)
    row_tiles, col_tiles = part // LANES, hidden // LANES
    for m, weight in enumerate((up, down)):

        def assemble(r, m=m, weight=weight):
            for k in range(col_tiles):
                n = map_ref[0, (m * row_tiles + r) * col_tiles + k]
                yn, zn, cn = n // (2 * side), (n // 2) % side, n % 2
                along = cn * (zn - yn)
                tile = arrived[cn * side + zn - along, yn + along]
                weight[pl.ds(pl.multiple_of(r * LANES, LANES), LANES), pl.ds(k * LANES, LANES)] = (
                    tile
                )

        each(row_tiles, assemble)

    rows_each = experts * slots // dps
    cut = rows_each // 2

    def to_hidden(i):
        wait_bytes(recv.at[i, pl.ds(0, experts - 1)], row_recv.at[i])
        rows = recv[i].reshape(experts * slots, part)
        product = jnp.dot(rows, up[...], preferred_element_type=jnp.float32)
        pre[i] = product.astype(jnp.bfloat16).reshape(dps, rows_each, hidden)
        top, low = pl.ds(0, cut), pl.ds(cut, cut)
        send(pre.at[i, far, top], half.at[i, 0], half_send.at[i], half_recv.at[i], me, right)
        send(pre.at[i, far, low], half.at[i, 1], half_send.at[i], half_recv.at[i], me, left)

    def relay(i):
        wait_bytes(half.at[i], half_recv.at[i])
        for k, (other, start) in enumerate(((right, 0), (left, cut))):
            piece = pl.ds(start, cut)
            total = pre[i, other, piece].astype(jnp.float32) + half[i, k].astype(jnp.float32)
            pre[i, other, piece] = total.astype(jnp.bfloat16)
            send(pre.at[i, other], sums.at[i, k], sum_send.at[i], sum_recv.at[i], me, other)

    def activate(i):
        wait_bytes(sums.at[i], sum_recv.at[i])
        total = pre[i, x].astype(jnp.float32)
        total = total + sums[i, 0].astype(jnp.float32) + sums[i, 1].astype(jnp.float32)
        hid[i, x] = (total * jax.nn.sigmoid(total)).astype(jnp.bfloat16)
        for other in (right, left):
            send(hid.at[i, x], hid.at[i, x], hid_send.at[i], hid_recv.at[i], me, other)

    def pass_on(i):
        wait_bytes(sums.at[i], hid_recv.at[i])
        for other, source, start in ((right, left, 0), (left, right, cut)):
            piece = hid.at[i, source, pl.ds(start, cut)]
            send(piece, piece, pass_send.at[i], pass_recv.at[i], me, other)

    def to_result(i):
        wait_bytes(half.at[i], pass_recv.at[i])
        units = hid[i].reshape(experts * slots, hidden)
        product = lax.dot_general(
            units, down[...], (((1,), (1,)), ((), ())), preferred_element_type=jnp.float32
        )
        res[i] = product.astype(jnp.bfloat16).reshape(experts, slots, part)

        def out(j):
            s = (as_source + 1 + j) % experts
            other = s // side
            slot = (z + other * (y - z)) * 2 + c
            send(res.at[i, s], ret.at[i, slot], ret_send.at[i], ret_recv.at[i], source_at(s), x)

        each(experts - 1, out)
        ret[i, as_expert] = res[i, as_source]

    def combine(i):
        wait_bytes(ret.at[i, pl.ds(0, experts - 1)], ret_recv.at[i])
        outs = ret[i].reshape(experts * slots, part)
        mixed = jnp.dot(comb_all[i], outs, preferred_element_type=jnp.float32)
        mix[pl.ds(i * blocks, blocks)] = mixed.astype(jnp.bfloat16).reshape(blocks, tok, part)

        def out(j):
            k = i * blocks + (j + x) % blocks

            @pl.when(k != mine)
            def _():
                send(mix.at[k], fin.at[mine], fin_send, fin_recv, line_at(k), k % dps)

        each(blocks, out)

    steps = (to_hidden, relay, activate, pass_on, to_result, combine)
    for turn in range(chunks + LAG[-1]):
        for step, late in sorted(zip(steps, LAG), key=lambda p: ORDER * p[1]):
            if 0 <= turn - late < chunks:
                step(turn - late)

    fin[mine] = mix[mine]
    wait_bytes(routers.at[pl.ds(0, dps - 1)], router_recv)
    wait_bytes(fin.at[pl.ds(0, line - 1)], fin_recv)
    squares = jnp.zeros((tok, 1), jnp.float32)
    for g in range(dps):
        total = fin[g].astype(jnp.float32)
        for other in range(1, side):
            total = total + fin[other * dps + g].astype(jnp.float32)
        columns = slice(g * part, (g + 1) * part)
        layer = (tokens_ref[:, columns].astype(jnp.float32) + total).astype(jnp.bfloat16)
        out_ref[:, columns] = layer
        stream = layer.astype(jnp.float32)
        squares = squares + jnp.sum(stream * stream, axis=1, keepdims=True)
    renorm = lax.rsqrt(squares / (dps * part) + 1e-06)
    logits = jnp.zeros((tok, scores_ref.shape[1]), jnp.float32)
    for g in range(dps):
        stream = out_ref[:, g * part : (g + 1) * part].astype(jnp.float32)
        normed = (stream * renorm).astype(jnp.bfloat16)
        logits = logits + jnp.dot(normed, routers[g], preferred_element_type=jnp.float32)
    scores_ref[...] = jax.nn.sigmoid(logits)

    wait_bytes(got.at[0, pl.ds(0, dps - 1)], gx_send)
    for d, step in ways:
        for k in range(last):
            block = got.at[0] if k + 1 < last else got.at[0, pl.ds(0, dps // 2)]
            wait_bytes(block, ag_send.at[d, k])
            for i in range(loads):
                wait_bytes(ins[k + 1].at[d, i], along_send.at[d, i, k])
        for i in range(loads):
            for k in range(1, over_hops(i)):
                wait_bytes(getattr(own_refs, f"over{i}").at[0, d], over_send.at[d, i, k - 1])
    wait_bytes(routers.at[pl.ds(0, dps - 1)], router_send)
    wait_bytes(arrived.at[pl.ds(0, experts - 1)], tile_send)
    wait_bytes(fin.at[pl.ds(0, line - 1)], fin_send)
    for i in range(chunks):
        wait_bytes(recv.at[i, pl.ds(0, experts - 1)], row_send.at[i])
        wait_bytes(half.at[i], half_send.at[i])
        wait_bytes(sums.at[i], sum_send.at[i])
        wait_bytes(sums.at[i], hid_send.at[i])
        wait_bytes(half.at[i], pass_send.at[i])
        wait_bytes(ret.at[i, pl.ds(0, experts - 1)], ret_send.at[i])


def vmem():
    return pl.BlockSpec(memory_space=pltpu.VMEM)


def per_device(side, tokens, norm_gain, router, next_router, expert_ids, store, send_list, cache_map):
    tok, width = tokens.shape
    dps = lax.axis_size("dp")
    experts = router.shape[1]
    top = expert_ids.shape[1]
    tiles = cache_map.shape[1]
    part = width // dps
    row_tiles = part // LANES
    hidden = tiles // (2 * row_tiles) * LANES
    line = side * dps
    chunks = min(PIECES, side)
    slots = line // chunks * CAP
    bf16 = jnp.bfloat16

    lanes = experts * CAP + -(experts * CAP) % LANES
    rows_all = 2 * side * slots
    shared = pltpu.VMEM((chunks, dps, rows_all // dps, hidden), bf16)
    paired = pltpu.VMEM((chunks, 2, rows_all // dps, hidden), bf16)
    halves = pltpu.VMEM((chunks, 2, rows_all // dps // 2, hidden), bf16)
    traded = pltpu.VMEM((chunks, 2 * side, slots, part), bf16)
    lined = pltpu.VMEM((line, tok, part), bf16)
    weight = pltpu.VMEM((part, hidden), bf16)
    pairs = hops_along(side)
    last = side // 2
    tile = (LANES, LANES)

    def sems(*shape):
        return pltpu.SemaphoreType.DMA(shape)

    scratch = [
        ("store", pltpu.VMEM((tiles, *tile), bf16)),
        ("mid", pltpu.VMEM((len(pairs), 2, 2, side, *tile), bf16)),
        ("arrived", pltpu.VMEM((2 * side, side, *tile), bf16)),
        ("up", weight),
        ("down", weight),
        ("got", pltpu.VMEM((side, dps, tok, part + lanes), bf16)),
        ("rows_out", traded),
        ("comb_all", pltpu.VMEM((chunks, line // chunks * tok, rows_all), bf16)),
        ("routers", pltpu.VMEM((dps, part, next_router.shape[1]), bf16)),
        ("recv", traded),
        ("pre", shared),
        ("half", halves),
        ("sums", paired),
        ("hid", shared),
        ("res", traded),
        ("ret", traded),
        ("mix", lined),
        ("fin", lined),
    ]
    scratch += [(f"one{k}", pltpu.SemaphoreType.DMA) for k in range(9)]
    scratch += [(f"many{k}", sems(chunks)) for k in range(12)]
    scratch += [(f"ring{k}", sems(2, last)) for k in range(2)]
    scratch += [(f"path{k}", sems(2, len(pairs), last)) for k in range(4)]
    scratch += [("out1", pltpu.VMEM((2, len(pairs), side - 1, 2, *tile), bf16))]
    scratch += [("pay", pltpu.VMEM((dps, tok, part + lanes), bf16))]
    for k in range(1, last + 1):
        scratch += [(f"in{k}", pltpu.VMEM((2, len(pairs), side + 1 - 2 * k, 2, *tile), bf16))]
    for i, (one_way, _) in enumerate(pairs):
        inner = (side,) if one_way == last else (2, side)
        scratch += [(f"over{i}", pltpu.VMEM((max(1, one_way - 1), 2, *inner, *tile), bf16))]
    return pl.pallas_call(
        functools.partial(
            layer_kernel, side, dps, chunks, tuple(name for name, _ in scratch)
        ),
        out_shape=(
            jax.ShapeDtypeStruct((tok, width), bf16),
            jax.ShapeDtypeStruct((tok, next_router.shape[1]), jnp.float32),
        ),
        in_specs=[vmem()] * 5
        + [pl.BlockSpec(memory_space=pltpu.SMEM)] * 2
        + [pl.BlockSpec(memory_space=pl.ANY)],
        out_specs=(vmem(), vmem()),
        scratch_shapes=[shape for _, shape in scratch],
        compiler_params=pltpu.CompilerParams(
            collective_id=0, has_side_effects=True, vmem_limit_bytes=60 << 20
        ),
    )(
        tokens,
        norm_gain[None],
        router,
        next_router,
        expert_ids.T,
        send_list,
        cache_map,
        store.reshape(tiles, LANES, LANES),
    )


def solution(mesh):
    side = round((mesh.shape["ep"] // 2) ** 0.5)
    in_specs = (
        P(("ep", "dp"), None),
        P(),
        P(),
        P("dp", None),
        P(("ep", "dp"), None),
        P("ep", "dp", None, None, None),
        P("ep", None),
        P("ep", None),
    )
    out_specs = (P(("ep", "dp"), None), P(("ep", "dp"), None))
    return jax.shard_map(
        functools.partial(per_device, side),
        mesh=mesh,
        in_specs=in_specs,
        out_specs=out_specs,
        check_vma=False,
    )
```

```python
import functools
import types

import jax
import jax.numpy as jnp
from jax import lax
from jax.experimental import pallas as pl
from jax.experimental.pallas import tpu as pltpu
from jax.sharding import PartitionSpec as P

MESH = pl.DeviceIdType.MESH
CAP = 2
LANES = 128
PIECES = 4
LAG = (0, 1, 2, 3, 4, 9)
ORDER = -1


def place(side):
    e = lax.axis_index("ep")
    x = lax.axis_index("dp")
    y, z, c = e // (2 * side), (e // 2) % side, e % 2
    a = y + c * (z - y)
    b = z + c * (y - z)
    return x, y, z, c, a, b


def on_line(side, a, b, c):
    wide, narrow = 2 * side - c * (2 * side - 2), 2 + c * (2 * side - 2)
    return a * wide + b * narrow


def send(src, dst, send_sem, recv_sem, ep, dp):
    pltpu.make_async_remote_copy(
        src_ref=src,
        dst_ref=dst,
        send_sem=send_sem,
        recv_sem=recv_sem,
        device_id={"ep": ep, "dp": dp},
        device_id_type=MESH,
    ).start()


def wait_bytes(ref, sem):
    pltpu.make_async_copy(ref, ref, sem).wait()


def greet(ep, dp):
    pl.semaphore_signal(
        pltpu.get_barrier_semaphore(), inc=1, device_id={"ep": ep, "dp": dp}, device_id_type=MESH
    )


def each(count, body):
    def step(j, carry):
        body(j)
        return carry

    lax.fori_loop(0, count, step, 0)


def hops_along(side):
    pairs = [(d, (side - d) % side) for d in range(side // 2 - 1, 0, -1)]
    pairs.insert(0, (side // 2, 0))
    return pairs


def layer_kernel(
    side,
    dps,
    chunks,
    names,
    tokens_ref,
    gain_ref,
    router_ref,
    next_ref,
    ids_ref,
    list_ref,
    map_ref,
    store_hbm,
    out_ref,
    scores_ref,
    *scratch,
):
    own_refs = types.SimpleNamespace(**dict(zip(names, scratch)))
    pay = own_refs.pay
    (store, mid, arrived, up, down, got, rows_out, comb_all, routers, recv) = scratch[:10]
    (pre, half, sums, hid, res, ret, mix, fin) = scratch[10:18]
    (store_sem, gx_send, gx_recv, router_send, router_recv, tile_send, tile_recv) = scratch[18:25]
    (fin_send, fin_recv, row_send, row_recv, half_send, half_recv) = scratch[25:31]
    (sum_send, sum_recv, hid_send, hid_recv, pass_send, pass_recv) = scratch[31:37]
    (ret_send, ret_recv, ag_send, ag_recv, along_send, along_recv) = scratch[37:43]
    (over_send, over_recv) = scratch[43:45]
    x, y, z, c, a, b = place(side)
    me = lax.axis_index("ep")
    line = side * dps
    mine = a * dps + x
    experts = 2 * side
    as_expert = b * 2 + c
    as_source = c * side + b
    part, hidden = up.shape
    slots = recv.shape[2]
    tok = tokens_ref.shape[0]
    blocks = line // chunks
    last = side // 2
    ways = ((0, 1), (1, side - 1))
    right, left, far = (x + 1) % dps, (x + dps - 1) % dps, (x + 2) % dps

    store_copy = pltpu.make_async_copy(store_hbm, store, store_sem)
    store_copy.start()

    def expert_at(d):
        return on_line(side, a, d // 2, c) + d % 2

    def source_at(s):
        other, i = s // side, s % side
        first = y * 2 * side + i * 2
        second = i * 2 * side + z * 2 + 1
        return first + other * (second - first)

    def line_at(k):
        return on_line(side, k // dps, b, c) + c

    def hello_experts(j):
        greet(expert_at((as_expert + 1 + j) % experts), x)

    def hello_sources(j):
        greet(source_at((as_source + 1 + j) % experts), x)

    def hello_line(j):
        k = (mine + 1 + j) % line
        greet(line_at(k), k % dps)

    each(experts - 1, hello_experts)
    each(experts - 1, hello_sources)
    each(line - 1, hello_line)

    def route():
        values = tokens_ref[...].astype(jnp.float32)
        scale = lax.rsqrt(jnp.mean(values * values, axis=1, keepdims=True) + 1e-06)
        normed = (values * scale * gain_ref[...]).astype(jnp.bfloat16)
        logits = jnp.dot(normed, router_ref[...], preferred_element_type=jnp.float32)
        scores = jax.nn.sigmoid(logits)
        count = scores.shape[1]
        top = ids_ref.shape[0]
        ids = lax.dot_general(
            (
                lax.broadcasted_iota(jnp.int32, (tok, tok), 0)
                == lax.broadcasted_iota(jnp.int32, (tok, tok), 1)
            ).astype(jnp.float32),
            ids_ref[...].astype(jnp.float32),
            (((1,), (1,)), ((), ())),
            preferred_element_type=jnp.float32,
        ).astype(jnp.int32)
        lane = lax.broadcasted_iota(jnp.int32, (tok, count), 1)
        hits = [(ids[:, k : k + 1] == lane).astype(jnp.float32) for k in range(top)]
        picked = [jnp.sum(hit * scores, axis=1, keepdims=True) for hit in hits]
        total = functools.reduce(jnp.add, picked)
        weights = [(2.5 * p / total).astype(jnp.bfloat16).astype(jnp.float32) for p in picked]
        weight = functools.reduce(jnp.add, [hit * w for hit, w in zip(hits, weights)])
        named = functools.reduce(jnp.add, hits)
        earlier = (
            lax.broadcasted_iota(jnp.int32, (tok, tok), 0)
            > lax.broadcasted_iota(jnp.int32, (tok, tok), 1)
        ).astype(jnp.float32)
        rank = jnp.dot(earlier, named, preferred_element_type=jnp.float32)
        lanes = pay.shape[2] - part
        e = lax.broadcasted_iota(jnp.int32, (count, lanes), 0)
        column = lax.broadcasted_iota(jnp.int32, (count, lanes), 1)
        ye, ze, ce = e // (2 * side), (e // 2) % side, e % 2
        turn_y, turn_z = ye + c * (ze - ye), ze + c * (ye - ze)
        first = (turn_y * (2 * side) + turn_z * 2 + ce) * CAP
        combine = jnp.zeros((tok, lanes), jnp.float32)
        for r in range(CAP):
            ranked = jnp.where(rank == r, weight, 0.0).astype(jnp.bfloat16)
            place_r = (column == first + r).astype(jnp.float32).astype(jnp.bfloat16)
            combine = combine + jnp.dot(ranked, place_r, preferred_element_type=jnp.float32)
        for g in range(dps):
            pay[g, :, :part] = normed[:, g * part : (g + 1) * part]
            pay[g, :, part:] = combine.astype(jnp.bfloat16)

    def tokens_out():
        def out(j):
            other = (x + 1 + j) % dps
            send(pay.at[other], got.at[a, x], gx_send, gx_recv, me, other)

        each(dps - 1, out)
        got[a, x] = pay[x]

    def tokens_step(k):
        if k == 0:
            wait_bytes(got.at[a, pl.ds(0, dps - 1)], gx_recv)
        else:
            for d, step in ways:
                block = got.at[0] if k < last else got.at[0, pl.ds(0, dps // 2)]
                wait_bytes(block, ag_recv.at[d, k - 1])
        if k == last:
            return
        for d, step in ways:
            origin = (a + side - k if d == 0 else a + k) % side
            block = got.at[origin]
            if k + 1 == last:
                block = got.at[origin, pl.ds(d * (dps // 2), dps // 2)]
            to = on_line(side, (a + step) % side, b, c) + c
            send(block, block, ag_send.at[d, k], ag_recv.at[d, k], to, x)

    pairs = hops_along(side)
    outs, ins = own_refs.out1, [None] + [getattr(own_refs, f"in{k}") for k in range(1, last + 1)]

    def tile_for(i, q, h, there):
        ep = on_line(side, there, (b + pairs[i][q]) % side, c) + h
        return store[jnp.maximum(list_ref[0, ep], 0)]

    def along_fill(i):
        for d, step in ways:

            def near(j, d=d):
                there = (a + 1 + j if d == 0 else a + side - 1 - j) % side
                for h in range(2):
                    for q in range(2):
                        outs[d, i, 2 * j + h, q] = tile_for(i, q, h, there)

            if last > 1:
                each(last - 1, near)
            for q in range(2):
                outs[d, i, 2 * (last - 1), q] = tile_for(i, q, d, (a + last) % side)
        for h in range(2):
            for q in range(2):
                mid[i, q, h, a] = tile_for(i, q, h, a)

    def along_start(i):
        for d, step in ways:
            to = on_line(side, (a + step) % side, b, c) + c
            send(outs.at[d, i], ins[1].at[d, i], along_send.at[d, i, 0], along_recv.at[d, i, 0], to, x)

    def along_step(i, k):
        for d, step in ways:
            wait_bytes(ins[k].at[d, i], along_recv.at[d, i, k - 1])
            if k < last:
                rest = ins[k].at[d, i, pl.ds(2, side - 1 - 2 * k)]
                to = on_line(side, (a + step) % side, b, c) + c
                send(
                    rest, ins[k + 1].at[d, i], along_send.at[d, i, k], along_recv.at[d, i, k], to, x
                )
        for d, step in ways:
            origin = (a + side - k if d == 0 else a + k) % side
            for h in (0, 1) if k < last else (d,):
                for q in range(2):
                    mid[i, q, h, origin] = ins[k][d, i, h if k < last else 0, q]

    def over_hops(i):
        return min(pairs[i][0], side - pairs[i][0])

    def over_step(i, k):
        hops = over_hops(i)
        split = hops == last
        trail = getattr(own_refs, f"over{i}")
        for d, step in ways:
            if k == 1:
                block = mid.at[i, 0, d] if split else mid.at[i, d]
            else:
                block = trail.at[k - 2, d]
                wait_bytes(block, over_recv.at[d, i, k - 2])
            to = on_line(side, a, (b + step) % side, c)
            origin = c * side + (b + side - k + 1 if d == 0 else b + k - 1) % side
            if k < hops:
                sems = over_send.at[d, i, k - 1], over_recv.at[d, i, k - 1]
                send(block, trail.at[k - 1, d], *sems, to + c, x)
            elif split:
                send(block, arrived.at[origin], tile_send, tile_recv, to + d, x)
            else:
                for h in range(2):
                    send(block.at[h], arrived.at[origin], tile_send, tile_recv, to + h, x)
        if split and k == 1:
            pair = me + 1 - 2 * c
            send(mid.at[i, 1, 1 - c], arrived.at[as_source], tile_send, tile_recv, pair, x)
            arrived[as_source] = mid[i, 1, c]

    def build_rows():
        depth = blocks * tok
        width = experts * slots
        lanes = got.shape[3] - part
        first = a * experts * CAP
        q = lax.broadcasted_iota(jnp.int32, (width, lanes), 0)
        k = lax.broadcasted_iota(jnp.int32, (width, lanes), 1)
        pick_t = (k == first + (q // slots) * CAP + q % CAP).astype(jnp.float32).astype(jnp.bfloat16)
        q = lax.broadcasted_iota(jnp.int32, (lanes, width), 1)
        k = lax.broadcasted_iota(jnp.int32, (lanes, width), 0)
        pick_n = (k == first + (q // slots) * CAP + q % CAP).astype(jnp.float32).astype(jnp.bfloat16)
        r = lax.broadcasted_iota(jnp.int32, (depth, width), 0)
        q = lax.broadcasted_iota(jnp.int32, (depth, width), 1)
        own = r // tok == (q % slots) // CAP
        r = lax.broadcasted_iota(jnp.int32, (width, depth), 1)
        q = lax.broadcasted_iota(jnp.int32, (width, depth), 0)
        own_t = r // tok == (q % slots) // CAP
        lines = got.shape[0] // chunks
        for i in range(chunks):
            piece = got[i * lines : (i + 1) * lines].reshape(depth, part + lanes)
            comb = piece[:, part:]
            spread = jnp.dot(comb, pick_n, preferred_element_type=jnp.float32)
            comb_all[i] = jnp.where(own, spread, 0.0).astype(jnp.bfloat16)
            spread_t = lax.dot_general(
                pick_t, comb, (((1,), (1,)), ((), ())), preferred_element_type=jnp.float32
            )
            named = jnp.where(own_t & (spread_t != 0.0), 1.0, 0.0).astype(jnp.bfloat16)
            rows = jnp.dot(named, piece[:, :part], preferred_element_type=jnp.float32)
            rows_out[i] = rows.astype(jnp.bfloat16).reshape(experts, slots, part)

    def rows_away(i):
        def out(j):
            d = (as_expert + 1 + j) % experts
            send(
                rows_out.at[i, d],
                recv.at[i, as_source],
                row_send.at[i],
                row_recv.at[i],
                expert_at(d),
                x,
            )

        each(experts - 1, out)
        recv[i, as_source] = rows_out[i, as_expert]

    def router_out(j):
        send(next_ref, routers.at[x], router_send, router_recv, me, (x + 1 + j) % dps)

    route()
    store_copy.wait()
    along_fill(0)
    pl.semaphore_wait(pltpu.get_barrier_semaphore(), 2 * (experts - 1) + line - 1)
    loads = len(pairs)
    late = min(1, loads - 1)
    for turn in range(loads + 2 * last):
        if turn < loads:
            along_start(turn)
        if turn + 1 < loads:
            along_fill(turn + 1)
        if turn == 0:
            tokens_out()
            each(dps - 1, router_out)
            routers[x] = next_ref[...]
        if late <= turn <= last + late:
            tokens_step(turn - late)
        for k in range(1, last + 1):
            if 0 <= turn - k < loads:
                along_step(turn - k, k)
        if turn == last + late:
            build_rows()
        for k in range(1, last + 1):
            i = turn - last - k + 1
            if 0 <= i < loads and k <= over_hops(i):
                if k == 1 and i == loads - 1:
                    rows_away(0)
                over_step(i, k)

    for i in range(1, chunks):
        rows_away(i)

    wait_bytes(arrived.at[pl.ds(0, experts - 1)], tile_recv)
    row_tiles, col_tiles = part // LANES, hidden // LANES

    def assemble(m, weight):
        def one_row(r):
            for k in range(col_tiles):
                n = map_ref[0, (m * row_tiles + r) * col_tiles + k]
                yn, zn, cn = n // (2 * side), (n // 2) % side, n % 2
                along = cn * (zn - yn)
                tile = arrived[cn * side + zn - along, yn + along]
                weight[pl.ds(pl.multiple_of(r * LANES, LANES), LANES), pl.ds(k * LANES, LANES)] = (
                    tile
                )

        each(row_tiles, one_row)

    assemble(0, up)
    rows_each = experts * slots // dps
    cut = rows_each // 2

    def to_hidden(i):
        wait_bytes(recv.at[i, pl.ds(0, experts - 1)], row_recv.at[i])
        rows = recv[i].reshape(experts * slots, part)
        product = jnp.dot(rows, up[...], preferred_element_type=jnp.float32)
        pre[i] = product.astype(jnp.bfloat16).reshape(dps, rows_each, hidden)
        top, low = pl.ds(0, cut), pl.ds(cut, cut)
        send(pre.at[i, far, top], half.at[i, 0], half_send.at[i], half_recv.at[i], me, right)
        send(pre.at[i, far, low], half.at[i, 1], half_send.at[i], half_recv.at[i], me, left)

    def relay(i):
        wait_bytes(half.at[i], half_recv.at[i])
        for k, (other, start) in enumerate(((right, 0), (left, cut))):
            piece = pl.ds(start, cut)
            total = pre[i, other, piece].astype(jnp.float32) + half[i, k].astype(jnp.float32)
            pre[i, other, piece] = total.astype(jnp.bfloat16)
            send(pre.at[i, other], sums.at[i, k], sum_send.at[i], sum_recv.at[i], me, other)

    def activate(i):
        wait_bytes(sums.at[i], sum_recv.at[i])
        total = pre[i, x].astype(jnp.float32)
        total = total + sums[i, 0].astype(jnp.float32) + sums[i, 1].astype(jnp.float32)
        hid[i, x] = (total * jax.nn.sigmoid(total)).astype(jnp.bfloat16)
        for other in (right, left):
            send(hid.at[i, x], hid.at[i, x], hid_send.at[i], hid_recv.at[i], me, other)

    def pass_on(i):
        wait_bytes(sums.at[i], hid_recv.at[i])
        for other, source, start in ((right, left, 0), (left, right, cut)):
            piece = hid.at[i, source, pl.ds(start, cut)]
            send(piece, piece, pass_send.at[i], pass_recv.at[i], me, other)

    def to_result(i):
        wait_bytes(half.at[i], pass_recv.at[i])
        units = hid[i].reshape(experts * slots, hidden)
        product = lax.dot_general(
            units, down[...], (((1,), (1,)), ((), ())), preferred_element_type=jnp.float32
        )
        res[i] = product.astype(jnp.bfloat16).reshape(experts, slots, part)

        def out(j):
            s = (as_source + 1 + j) % experts
            other = s // side
            slot = (z + other * (y - z)) * 2 + c
            send(res.at[i, s], ret.at[i, slot], ret_send.at[i], ret_recv.at[i], source_at(s), x)

        each(experts - 1, out)
        ret[i, as_expert] = res[i, as_source]

    def combine(i):
        wait_bytes(ret.at[i, pl.ds(0, experts - 1)], ret_recv.at[i])
        outs = ret[i].reshape(experts * slots, part)
        mixed = jnp.dot(comb_all[i], outs, preferred_element_type=jnp.float32)
        mix[pl.ds(i * blocks, blocks)] = mixed.astype(jnp.bfloat16).reshape(blocks, tok, part)

        def out(j):
            k = i * blocks + (j + x) % blocks

            @pl.when(k != mine)
            def _():
                send(mix.at[k], fin.at[mine], fin_send, fin_recv, line_at(k), k % dps)

        each(blocks, out)

    steps = (to_hidden, relay, activate, pass_on, to_result, combine)
    for turn in range(chunks + LAG[-1]):
        for step, late in sorted(zip(steps, LAG), key=lambda p: ORDER * p[1]):
            if 0 <= turn - late < chunks:
                step(turn - late)
        if turn == 0:
            assemble(1, down)

    fin[mine] = mix[mine]
    wait_bytes(routers.at[pl.ds(0, dps - 1)], router_recv)
    wait_bytes(fin.at[pl.ds(0, line - 1)], fin_recv)
    squares = jnp.zeros((tok, 1), jnp.float32)
    for g in range(dps):
        total = fin[g].astype(jnp.float32)
        for other in range(1, side):
            total = total + fin[other * dps + g].astype(jnp.float32)
        columns = slice(g * part, (g + 1) * part)
        layer = (tokens_ref[:, columns].astype(jnp.float32) + total).astype(jnp.bfloat16)
        out_ref[:, columns] = layer
        stream = layer.astype(jnp.float32)
        squares = squares + jnp.sum(stream * stream, axis=1, keepdims=True)
    renorm = lax.rsqrt(squares / (dps * part) + 1e-06)
    logits = jnp.zeros((tok, scores_ref.shape[1]), jnp.float32)
    for g in range(dps):
        stream = out_ref[:, g * part : (g + 1) * part].astype(jnp.float32)
        normed = (stream * renorm).astype(jnp.bfloat16)
        logits = logits + jnp.dot(normed, routers[g], preferred_element_type=jnp.float32)
    scores_ref[...] = jax.nn.sigmoid(logits)

    wait_bytes(got.at[0, pl.ds(0, dps - 1)], gx_send)
    for d, step in ways:
        for k in range(last):
            block = got.at[0] if k + 1 < last else got.at[0, pl.ds(0, dps // 2)]
            wait_bytes(block, ag_send.at[d, k])
            for i in range(loads):
                wait_bytes(ins[k + 1].at[d, i], along_send.at[d, i, k])
        for i in range(loads):
            for k in range(1, over_hops(i)):
                wait_bytes(getattr(own_refs, f"over{i}").at[0, d], over_send.at[d, i, k - 1])
    wait_bytes(routers.at[pl.ds(0, dps - 1)], router_send)
    wait_bytes(arrived.at[pl.ds(0, experts - 1)], tile_send)
    wait_bytes(fin.at[pl.ds(0, line - 1)], fin_send)
    for i in range(chunks):
        wait_bytes(recv.at[i, pl.ds(0, experts - 1)], row_send.at[i])
        wait_bytes(half.at[i], half_send.at[i])
        wait_bytes(sums.at[i], sum_send.at[i])
        wait_bytes(sums.at[i], hid_send.at[i])
        wait_bytes(half.at[i], pass_send.at[i])
        wait_bytes(ret.at[i, pl.ds(0, experts - 1)], ret_send.at[i])


def vmem():
    return pl.BlockSpec(memory_space=pltpu.VMEM)


def per_device(side, tokens, norm_gain, router, next_router, expert_ids, store, send_list, cache_map):
    tok, width = tokens.shape
    dps = lax.axis_size("dp")
    experts = router.shape[1]
    top = expert_ids.shape[1]
    tiles = cache_map.shape[1]
    part = width // dps
    row_tiles = part // LANES
    hidden = tiles // (2 * row_tiles) * LANES
    line = side * dps
    chunks = min(PIECES, side)
    slots = line // chunks * CAP
    bf16 = jnp.bfloat16

    lanes = experts * CAP + -(experts * CAP) % LANES
    rows_all = 2 * side * slots
    shared = pltpu.VMEM((chunks, dps, rows_all // dps, hidden), bf16)
    paired = pltpu.VMEM((chunks, 2, rows_all // dps, hidden), bf16)
    halves = pltpu.VMEM((chunks, 2, rows_all // dps // 2, hidden), bf16)
    traded = pltpu.VMEM((chunks, 2 * side, slots, part), bf16)
    lined = pltpu.VMEM((line, tok, part), bf16)
    weight = pltpu.VMEM((part, hidden), bf16)
    pairs = hops_along(side)
    last = side // 2
    tile = (LANES, LANES)

    def sems(*shape):
        return pltpu.SemaphoreType.DMA(shape)

    scratch = [
        ("store", pltpu.VMEM((tiles, *tile), bf16)),
        ("mid", pltpu.VMEM((len(pairs), 2, 2, side, *tile), bf16)),
        ("arrived", pltpu.VMEM((2 * side, side, *tile), bf16)),
        ("up", weight),
        ("down", weight),
        ("got", pltpu.VMEM((side, dps, tok, part + lanes), bf16)),
        ("rows_out", traded),
        ("comb_all", pltpu.VMEM((chunks, line // chunks * tok, rows_all), bf16)),
        ("routers", pltpu.VMEM((dps, part, next_router.shape[1]), bf16)),
        ("recv", traded),
        ("pre", shared),
        ("half", halves),
        ("sums", paired),
        ("hid", shared),
        ("res", traded),
        ("ret", traded),
        ("mix", lined),
        ("fin", lined),
    ]
    scratch += [(f"one{k}", pltpu.SemaphoreType.DMA) for k in range(9)]
    scratch += [(f"many{k}", sems(chunks)) for k in range(12)]
    scratch += [(f"ring{k}", sems(2, last)) for k in range(2)]
    scratch += [(f"path{k}", sems(2, len(pairs), last)) for k in range(4)]
    scratch += [("out1", pltpu.VMEM((2, len(pairs), side - 1, 2, *tile), bf16))]
    scratch += [("pay", pltpu.VMEM((dps, tok, part + lanes), bf16))]
    for k in range(1, last + 1):
        scratch += [(f"in{k}", pltpu.VMEM((2, len(pairs), side + 1 - 2 * k, 2, *tile), bf16))]
    for i, (one_way, _) in enumerate(pairs):
        inner = (side,) if one_way == last else (2, side)
        scratch += [(f"over{i}", pltpu.VMEM((max(1, one_way - 1), 2, *inner, *tile), bf16))]
    return pl.pallas_call(
        functools.partial(
            layer_kernel, side, dps, chunks, tuple(name for name, _ in scratch)
        ),
        out_shape=(
            jax.ShapeDtypeStruct((tok, width), bf16),
            jax.ShapeDtypeStruct((tok, next_router.shape[1]), jnp.float32),
        ),
        in_specs=[vmem()] * 5
        + [pl.BlockSpec(memory_space=pltpu.SMEM)] * 2
        + [pl.BlockSpec(memory_space=pl.ANY)],
        out_specs=(vmem(), vmem()),
        scratch_shapes=[shape for _, shape in scratch],
        compiler_params=pltpu.CompilerParams(
            collective_id=0, has_side_effects=True, vmem_limit_bytes=60 << 20
        ),
    )(
        tokens,
        norm_gain[None],
        router,
        next_router,
        expert_ids.T,
        send_list,
        cache_map,
        store.reshape(tiles, LANES, LANES),
    )


def solution(mesh):
    side = round((mesh.shape["ep"] // 2) ** 0.5)
    in_specs = (
        P(("ep", "dp"), None),
        P(),
        P(),
        P("dp", None),
        P(("ep", "dp"), None),
        P("ep", "dp", None, None, None),
        P("ep", None),
        P("ep", None),
    )
    out_specs = (P(("ep", "dp"), None), P(("ep", "dp"), None))
    return jax.shard_map(
        functools.partial(per_device, side),
        mesh=mesh,
        in_specs=in_specs,
        out_specs=out_specs,
        check_vma=False,
    )
```
